32 devices in a mesh: dp: 4 (over z), ctx: 4 (over y, core), tp: 2 (over x).
Axes of the slice: x: 2, y: 2, z: 4, core: 2. Of those that a mesh axis runs over, the one named last changes fastest.
Arguments:
- hidden: bfloat16 [4, 512, 4096], P('dp', 'ctx'), may hold values from -6 to 6
- query_heads: bfloat16 [4, 512, 4096], P('dp', 'ctx', 'tp'), may hold values from -6 to 6
- key_heads: bfloat16 [4, 512, 512], P('dp', 'ctx', 'tp'), may hold values from -6 to 6
- value_heads: bfloat16 [4, 512, 512], P('dp', 'ctx', 'tp'), may hold values from -6 to 6
- attention_out: bfloat16 [4, 512, 4096], P('dp', 'ctx', 'tp'), may hold values from -3 to 3
- output_grad: bfloat16 [4, 512, 4096], P('dp', 'ctx', 'tp'), may hold values from -3 to 3
- log_norm: float32 [4, 32, 512], P('dp', 'tp', 'ctx'), may hold values from -40 to 40, as said below
- block_order: int32 [8], replicated, may hold values from 0 to 7, as said below
- value_weight: bfloat16 [4096, 512], P(None, 'tp'), may hold values from -0.25 to 0.25
Outputs:
- query_grad: bfloat16 [4, 512, 4096], P('dp', 'ctx', 'tp')
- key_grad: bfloat16 [4, 512, 512], P('dp', 'ctx', 'tp')
- value_grad: bfloat16 [4, 512, 512], P('dp', 'ctx', 'tp')
- hidden_grad: bfloat16 [4, 512, 4096], P('dp', 'ctx', 'tp')
- weight_grad: float32 [4096, 512], P('ctx', 'tp')
The draws below stay inside these ranges and needn't reach their ends.
Inputs may be any that keep to these rules, and one draw needn't show every extreme that they name: `block_order`: each of 0 to 7 once. log_norm is the log of the sum of exp(scores) over the keys visible to that row, so the probabilities of each row and head sum to one.
All inputs are finite; a program needn't handle non-finite values.
Results may differ from the reference program's by a relative error of at most 0.025.
Values may be sent and summed in bfloat16 or wider, within the bound.
A program may use at most 64 MiB of HBM per device.

```python
import jax
import jax.numpy as jnp
from jax import lax

D = 4096
HD = 128
HQ = 32
KVH = 4
TOK_DEV = 128
SEQS = 4
LEN = 512
BLK = 64
NBLK = 8
N_CTX = 4


def attention_inputs(key):
    block_perm = jax.random.permutation(jax.random.fold_in(key, 501), NBLK).astype(jnp.int32)
    query_shape = (SEQS, LEN, HQ * HD)
    key_shape = (SEQS, LEN, KVH * HD)
    query_vals = jax.random.truncated_normal(jax.random.fold_in(key, 502), -6.0, 6.0, query_shape, jnp.float32)
    key_vals = jax.random.truncated_normal(jax.random.fold_in(key, 503), -6.0, 6.0, key_shape, jnp.float32)
    return (block_perm, query_vals.astype(jnp.bfloat16), key_vals.astype(jnp.bfloat16))


def draw_block_order(key, part):
    block_perm, query_vals, key_vals = attention_inputs(key)
    return block_perm


def draw_query_heads(key, part):
    block_perm, query_vals, key_vals = attention_inputs(key)
    return query_vals


def draw_key_heads(key, part):
    block_perm, query_vals, key_vals = attention_inputs(key)
    return key_vals


def draw_log_norm(key, part):
    block_perm, query_vals, key_vals = attention_inputs(key)
    row_ids = jnp.arange(LEN, dtype=jnp.int32)
    positions = block_perm[row_ids // BLK] * BLK + row_ids % BLK
    visible = positions[None, :] <= positions[:, None]
    members = HQ // KVH
    grouped = query_vals.astype(jnp.float32).reshape(SEQS, LEN, KVH, members, HD).transpose(0, 2, 3, 1, 4).reshape(SEQS * KVH, members, LEN, HD)
    keyed = key_vals.astype(jnp.float32).reshape(SEQS, LEN, KVH, HD).transpose(0, 2, 1, 3).reshape(SEQS * KVH, LEN, HD)

    def normalizer(pair):
        scores = jnp.einsum('jte,ke->jtk', pair[0], pair[1]) * HD ** (-0.5)
        return jax.scipy.special.logsumexp(jnp.where(visible[None], scores, -jnp.inf), axis=-1)
    return lax.map(normalizer, (grouped, keyed)).reshape(SEQS, HQ, LEN)


def strengthened(result, key, source, target, shards_of, factor):
    def block_of(dim):
        return (jnp.arange(result.shape[dim]) // (result.shape[dim] // shards_of)).reshape((-1,) + (1,) * (result.ndim - 1 - dim))

    near = jax.random.permutation(key, shards_of)[block_of(target)]
    second = (block_of(target) + shards_of // 2) % shards_of
    return jnp.where((block_of(source) == near) | (block_of(source) == second), factor * result, result)


def shard_levels(rng, extent, pieces, least, high):
    def one(dim, blocks):
        heights = jax.random.uniform(jax.random.fold_in(jax.random.fold_in(rng, 6), dim), (blocks,), jnp.float32, least / len(pieces), high / len(pieces))
        return jnp.repeat(jnp.exp(heights), extent[dim] // blocks).reshape((-1,) + (1,) * (len(extent) - dim - 1))

    loudness = one(*pieces[0])
    for cut in pieces[1:]:
        loudness = loudness * one(*cut)
    return loudness


def centred(stream_key, shape, spread, reach, pieces=(), kind=jnp.bfloat16):
    loudness = shard_levels(stream_key, shape, pieces, -0.22, 0.18) if pieces else 1.0
    drawn = jax.random.normal(stream_key, shape, jnp.float32) * spread * loudness
    return jnp.minimum(jnp.maximum(drawn, -reach), reach).astype(kind)


def bell_draw_with(own_key, extent, spread, reach, cuts, heavy, kind=jnp.bfloat16):
    values = spread * jax.random.normal(own_key, extent, jnp.float32)
    if cuts:
        values = values * shard_levels(own_key, extent, cuts, -0.22, 0.18)
    return jnp.clip(strengthened(values, jax.random.fold_in(own_key, 3), *heavy), -reach, reach).astype(kind)


def setup_inputs(seed: int = 0) -> dict:
    arg_keys = jax.random.split(jax.random.key(seed), 10)
    return {
        "hidden": bell_draw_with(arg_keys[0], (SEQS, LEN, D), 1.0, 6.0, ((0, 4), (1, 4)), (1, 2, 4, 2.0)),
        "query_heads": draw_query_heads(jax.random.fold_in(arg_keys[9], 71), 0),
        "key_heads": draw_key_heads(jax.random.fold_in(arg_keys[9], 71), 0),
        "value_heads": centred(arg_keys[3], (SEQS, LEN, KVH * HD), 1.0, 6.0, ((0, 4), (1, 4), (2, 2))),
        "attention_out": centred(arg_keys[4], (SEQS, LEN, HQ * HD), 0.5, 3.0, ((0, 4), (1, 4), (2, 2))),
        "output_grad": centred(arg_keys[5], (SEQS, LEN, HQ * HD), 0.5, 3.0, ((0, 4), (1, 4), (2, 2))),
        "log_norm": draw_log_norm(jax.random.fold_in(arg_keys[9], 71), 0),
        "block_order": draw_block_order(jax.random.fold_in(arg_keys[9], 71), 0),
        "value_weight": centred(arg_keys[8], (D, KVH * HD), (KVH * HD) ** -0.5, 0.25, ((1, 2),)),
    }


def storage_positions(block_order):
    row_ids = jnp.arange(LEN, dtype=jnp.int32)
    return block_order[row_ids // BLK] * BLK + row_ids % BLK


def reference(hidden, query_heads, key_heads, value_heads, attention_out, output_grad, log_norm, block_order, value_weight):
    positions = storage_positions(block_order)
    visible = positions[None, :] <= positions[:, None]
    members = HQ // KVH
    score_scale = HD ** -0.5

    def by_group(array):
        return array.astype(jnp.float32).reshape(SEQS, LEN, KVH, members, HD).transpose(0, 2, 3, 1, 4).reshape(SEQS * KVH, members, LEN, HD)

    def by_head(array):
        return array.astype(jnp.float32).reshape(SEQS, LEN, KVH, HD).transpose(0, 2, 1, 3).reshape(SEQS * KVH, LEN, HD)

    def pair_grads(items):
        queries, keys_f, values_f, outs_f, grads_f, norms_f = items
        scores = jnp.einsum('jte,ke->jtk', queries, keys_f) * score_scale
        probability = jnp.exp(jnp.where(visible[None], scores - norms_f[:, :, None], -jnp.inf))
        weights = lax.optimization_barrier(probability.astype(jnp.bfloat16)).astype(jnp.float32)
        row_delta = jnp.sum(grads_f * outs_f, axis=-1)
        value_part = jnp.einsum('jtk,jte->ke', weights, grads_f)
        through = jnp.einsum('jte,ke->jtk', grads_f, values_f)
        slopes = lax.optimization_barrier((probability * (through - row_delta[:, :, None])).astype(jnp.bfloat16)).astype(jnp.float32)
        query_part = score_scale * jnp.einsum('jtk,ke->jte', slopes, keys_f)
        key_part = score_scale * jnp.einsum('jtk,jte->ke', slopes, queries)
        return query_part, key_part, value_part

    query_parts, key_parts, value_parts = lax.map(pair_grads, (by_group(query_heads), by_head(key_heads), by_head(value_heads), by_group(attention_out), by_group(output_grad), log_norm.reshape(SEQS * KVH, members, LEN)))
    query_grad = query_parts.reshape(SEQS, KVH, members, LEN, HD).transpose(0, 3, 1, 2, 4).reshape(SEQS, LEN, HQ * HD).astype(jnp.bfloat16)
    key_grad = key_parts.reshape(SEQS, KVH, LEN, HD).transpose(0, 2, 1, 3).reshape(SEQS, LEN, KVH * HD).astype(jnp.bfloat16)
    value_grad = value_parts.reshape(SEQS, KVH, LEN, HD).transpose(0, 2, 1, 3).reshape(SEQS, LEN, KVH * HD).astype(jnp.bfloat16)
    flat_value = value_grad.reshape(SEQS * LEN, KVH * HD)
    hidden_grad = jnp.dot(flat_value, value_weight.T, preferred_element_type=jnp.float32).astype(jnp.bfloat16).reshape(SEQS, LEN, D)
    pieces_in = hidden.reshape(SEQS * N_CTX, TOK_DEV, D)
    pieces_grad = value_grad.reshape(SEQS * N_CTX, TOK_DEV, KVH * HD)

    def add_piece(summed, pair):
        partial_value = jnp.dot(pair[0].T, pair[1], preferred_element_type=jnp.float32)
        rounded = lax.optimization_barrier(partial_value.astype(jnp.bfloat16))
        return summed + rounded.astype(jnp.float32), None

    summed, unused = lax.scan(add_piece, jnp.zeros((D, KVH * HD), jnp.float32), (pieces_in, pieces_grad))
    weight_grad = summed * (SEQS * LEN) ** -0.5
    return query_grad, key_grad, value_grad, hidden_grad, weight_grad
```

```python
import functools

import jax
import jax.numpy as jnp
from jax import lax
from jax.experimental import pallas as pl
from jax.experimental.pallas import tpu as pltpu
from jax.sharding import PartitionSpec as P

HD = 128
HQ = 32
KVH = 4
F32 = jnp.float32
BF16 = jnp.bfloat16
MESH = pl.DeviceIdType.MESH


def dot(a, b, ca, cb):
    return lax.dot_general(a, b, (((ca,), (cb,)), ((), ())), preferred_element_type=F32)


def kernel(
    sizes,
    order_ref, k_ref, v_ref, norm_ref, hid_ref, q_ref, ao_ref, og_ref, vw_ref,
    dq_ref, dk_ref, dv_ref, dh_ref, dw_ref,
    qs, aos, ogs, kg, vg, hg, wg, ht, prob, acck, accv, bias,
    dvp, dvr, vown, vall, vtp, dkp, dkr, wp, zr, zown, zall,
    local_sem, send, recv,
):
    n, t, z, rows, groups, members, dn, dt, chunk, keyc = sizes
    me, mt, mz = lax.axis_index("ctx"), lax.axis_index("tp"), lax.axis_index("dp")
    keys = n * rows
    blk = rows // 2
    scale = HD ** (-0.5)
    width = 2 * rows
    pairs = members // 2

    loads = [
        pltpu.make_async_copy(q_ref, qs, local_sem.at[0]),
        pltpu.make_async_copy(og_ref, ogs, local_sem.at[1]),
        pltpu.make_async_copy(ao_ref, aos, local_sem.at[2]),
        pltpu.make_async_copy(
            hid_ref.at[0, :, pl.ds(pl.multiple_of(me * dn, 128), dn)], hg.at[me], local_sem.at[3]
        ),
        pltpu.make_async_copy(
            vw_ref.at[pl.ds(pl.multiple_of(mt * dt, 128), dt)], wg.at[mt], local_sem.at[4]
        ),
    ]
    for load in loads:
        load.start()

    peers = {"ctx": (me, n), "tp": (mt, t), "dp": (mz, z)}

    def others(axis):
        mine, count = peers[axis]
        return [lax.rem(mine + o, count) for o in range(1, count)]

    barrier = pltpu.get_barrier_semaphore()
    for axis in peers:
        for peer in others(axis):
            pl.semaphore_signal(barrier, inc=1, device_id={axis: peer}, device_id_type=MESH)
    pl.semaphore_wait(barrier, n - 1 + t - 1 + z - 1)

    used = [0]

    def fan(axis, source, target):
        made = []
        for o, peer in enumerate(others(axis)):
            copy = pltpu.make_async_remote_copy(
                src_ref=source(peer),
                dst_ref=target(o),
                send_sem=send.at[used[0]],
                recv_sem=recv.at[used[0]],
                device_id={axis: peer},
                device_id_type=MESH,
            )
            used[0] += 1
            copy.start()
            made.append(copy)
        return made

    my_rows = pl.ds(pl.multiple_of(me * rows, rows), rows)
    k_copies = fan("ctx", lambda p: k_ref.at[0], lambda o: kg.at[my_rows])
    v_copies = fan("ctx", lambda p: v_ref.at[0], lambda o: vg.at[my_rows])
    h_copies = fan(
        "ctx",
        lambda p: hid_ref.at[0, :, pl.ds(pl.multiple_of(p * dn, 128), dn)],
        lambda o: hg.at[me],
    )
    w_copies = fan(
        "tp", lambda p: vw_ref.at[pl.ds(pl.multiple_of(p * dt, 128), dt)], lambda o: wg.at[mt]
    )
    kg[my_rows] = k_ref[0]
    vg[my_rows] = v_ref[0]

    lane = lax.broadcasted_iota(jnp.int32, (blk, width), 1) % rows
    first = order_ref[2 * me] * blk
    second = order_ref[2 * me + 1] * blk
    query_pos = lane % blk + jnp.where(lane < blk, first, second)
    inside = lax.broadcasted_iota(jnp.int32, (blk, width), 0)
    for b in range(keys // blk):
        key_pos = inside + order_ref[b] * blk
        bias[b * blk : (b + 1) * blk] = jnp.where(key_pos <= query_pos, 0.0, -1e30).astype(F32)

    def two(ref, head):
        return jnp.concatenate(
            [ref[0, :, pl.ds(pl.multiple_of((head + j) * HD, HD), HD)] for j in range(2)], axis=0
        )

    def lanes(head):
        pieces = [norm_ref[0, pl.ds(head + j, 1), :] for j in range(2)]
        return jnp.concatenate(pieces, axis=1)

    loads[0].wait()
    loads[1].wait()
    for copy in k_copies:
        copy.wait_recv()

    def values(g):
        col = g * HD

        def pair(step, carry):
            head = g * members + step * 2
            q2, og2, norm = two(qs, head), two(ogs, head), lanes(head)

            def block(c, carry):
                at = pl.ds(pl.multiple_of(c * keyc, keyc), keyc)
                s = dot(kg[at, col : col + HD], q2, 1, 1) * scale
                p = jnp.exp(s + bias[at] - norm)
                prob[g * pairs + step, at] = p
                accv[g, at] += dot(p.astype(BF16), og2, 1, 0)
                return carry

            return lax.fori_loop(0, keys // keyc, block, carry)

        accv[g] = jnp.zeros((keys, HD), F32)
        lax.fori_loop(0, pairs, pair, 0)
        for s in range(n):
            dvp[g, s] = accv[g, s * rows : (s + 1) * rows].astype(BF16)
        return fan("ctx", lambda p: dvp.at[g, p], lambda o: dvr.at[g, o])

    def slopes(g):
        col = g * HD
        acck[g] = jnp.zeros((keys, HD), F32)

        def pair(step, carry):
            head = g * members + step * 2
            q2, og2 = two(qs, head), two(ogs, head)
            product = og2.astype(F32) * two(aos, head).astype(F32)
            delta = jnp.sum(product.T, axis=0, keepdims=True)

            def block(c, dq):
                at = pl.ds(pl.multiple_of(c * keyc, keyc), keyc)
                through = dot(vg[at, col : col + HD], og2, 1, 1)
                ds = (prob[g * pairs + step, at] * (through - delta)).astype(BF16)
                acck[g, at] += dot(ds, q2, 1, 0)
                return dq + dot(kg[at, col : col + HD].T, ds, 1, 0)

            dq = lax.fori_loop(0, keys // keyc, block, jnp.zeros((HD, width), F32))
            dq = (dq * scale).T.astype(BF16)
            for j in range(2):
                dq_ref[0, :, pl.ds(pl.multiple_of((head + j) * HD, HD), HD)] = dq[
                    j * rows : (j + 1) * rows
                ]
            return carry

        lax.fori_loop(0, pairs, pair, 0)
        for s in range(n):
            dkp[g, s] = acck[g, s * rows : (s + 1) * rows].astype(BF16)
        return fan("ctx", lambda p: dkp.at[g, p], lambda o: dkr.at[g, o])

    def reduced(copies, own, landed, g):
        for copy in copies:
            copy.wait_recv()
        total = own
        for o in range(n - 1):
            total = total + landed[g, o].astype(F32)
        return total

    def value_out(g, copies):
        col = g * HD
        total = reduced(copies, dvp[g, me].astype(F32), dvr, g).astype(BF16)
        dv_ref[0, :, col : col + HD] = total
        vown[g] = total
        made = fan("ctx", lambda p: vown.at[g], lambda o: vall.at[g, me])
        made_tp = fan("tp", lambda p: vown.at[g], lambda o: vtp.at[g, mt])
        vall[g, me] = total
        vtp[g, mt] = total
        return made, made_tp

    def weight_part(g, copies):
        for copy in copies:
            copy.wait_recv()
        size = min(dn, 256)

        def tile(i, carry):
            at = pl.ds(pl.multiple_of(i * size, size), size)
            rhs = vall[g].reshape(keys, HD)
            wp[g, at] = dot(ht[at], rhs, 1, 0).astype(BF16)
            return carry

        lax.fori_loop(0, dn // size, tile, 0)
        if z * chunk > dn:
            wp[g, dn:] = jnp.zeros((z * chunk - dn, HD), BF16)

        def piece(p):
            return wp.at[g, pl.ds(pl.multiple_of(p * chunk, 16), chunk)]

        return fan("dp", piece, lambda o: zr.at[g, o])

    def weight_sum(g, copies):
        for copy in copies:
            copy.wait_recv()
        mine = pl.ds(pl.multiple_of(mz * chunk, 16), chunk)
        total = wp[g, mine].astype(F32)
        for o in range(z - 1):
            total = total + zr[g, o].astype(F32)
        total = total.astype(BF16)
        zown[g] = total
        made = fan("dp", lambda p: zown.at[g], lambda o: zall.at[g, mine])
        zall[g, mine] = total
        return made

    dv_copies = [values(g) for g in range(groups)]
    gathers, shares, dk_copies, w_parts = [], [], [], []
    loads[2].wait()
    for copy in v_copies:
        copy.wait_recv()
    made, made_tp = value_out(0, dv_copies[0])
    gathers.append(made)
    shares.append(made_tp)
    dk_copies.append(slopes(0))
    for g in range(1, groups):
        made, made_tp = value_out(g, dv_copies[g])
        gathers.append(made)
        shares.append(made_tp)
    loads[3].wait()
    for copy in h_copies:
        copy.wait_recv()
    for s in range(n):
        ht[:, s * rows : (s + 1) * rows] = hg[s].T
    w_parts.append(weight_part(0, gathers[0]))
    for g in range(1, groups):
        w_parts.append(weight_part(g, gathers[g]))
    for g in range(1, groups):
        dk_copies.append(slopes(g))
    z_copies = [weight_sum(g, w_parts[g]) for g in range(groups)]

    loads[4].wait()
    for copy in w_copies:
        copy.wait_recv()
    for g in range(groups):
        for copy in shares[g]:
            copy.wait_recv()
    size = min(dt, 256)

    def out_tile(i, carry):
        at = pl.ds(pl.multiple_of(i * size, size), size)
        total = jnp.zeros((rows, size), F32)
        for p in range(t):
            lhs = jnp.concatenate([vtp[g, p] for g in range(groups)], axis=1)
            total = total + dot(lhs, wg[p, at], 1, 1)
        dh_ref[0, :, at] = total.astype(BF16)
        return carry

    lax.fori_loop(0, dt // size, out_tile, 0)

    for g in range(groups):
        col = g * HD
        total = reduced(dk_copies[g], dkp[g, me].astype(F32), dkr, g)
        dk_ref[0, :, col : col + HD] = (total * scale).astype(BF16)

    token_norm = (z * n * rows) ** (-0.5)
    for g in range(groups):
        for copy in z_copies[g]:
            copy.wait_recv()
        dw_ref[:, g * HD : (g + 1) * HD] = zall[g, :dn].astype(F32) * token_norm

    everything = k_copies + v_copies + h_copies + w_copies
    for group in dv_copies + gathers + shares + dk_copies + w_parts + z_copies:
        everything = everything + group
    for copy in everything:
        copy.wait_send()


def shards(
    hidden, query_heads, key_heads, value_heads, attention_out, output_grad,
    log_norm, block_order, value_weight,
):
    n, t, z = lax.axis_size("ctx"), lax.axis_size("tp"), lax.axis_size("dp")
    rows = query_heads.shape[1]
    depth = hidden.shape[2]
    cols = key_heads.shape[2]
    groups = cols // HD
    heads = query_heads.shape[2] // HD
    members = heads // groups
    dn, dt = depth // n, depth // t
    chunk = -(-dn // (16 * z)) * 16
    keys = n * rows
    keyc = min(keys, 512)
    sizes = (n, t, z, rows, groups, members, dn, dt, chunk, keyc)
    count = (n - 1) * (3 + 3 * groups) + (t - 1) * (1 + groups) + (z - 1) * 2 * groups
    vmem, anywhere = pl.BlockSpec(memory_space=pltpu.VMEM), pl.BlockSpec(memory_space=pl.ANY)
    smem = pl.BlockSpec(memory_space=pltpu.SMEM)
    wide = (1, rows, heads * HD)
    scratch = [
        pltpu.VMEM(wide, BF16),
        pltpu.VMEM(wide, BF16),
        pltpu.VMEM(wide, BF16),
        pltpu.VMEM((keys, cols), BF16),
        pltpu.VMEM((keys, cols), BF16),
        pltpu.VMEM((n, rows, dn), BF16),
        pltpu.VMEM((t, dt, cols), BF16),
        pltpu.VMEM((dn, keys), BF16),
        pltpu.VMEM((heads // 2, keys, 2 * rows), F32),
        pltpu.VMEM((groups, keys, HD), F32),
        pltpu.VMEM((groups, keys, HD), F32),
        pltpu.VMEM((keys, 2 * rows), F32),
        pltpu.VMEM((groups, n, rows, HD), BF16),
        pltpu.VMEM((groups, n - 1, rows, HD), BF16),
        pltpu.VMEM((groups, rows, HD), BF16),
        pltpu.VMEM((groups, n, rows, HD), BF16),
        pltpu.VMEM((groups, t, rows, HD), BF16),
        pltpu.VMEM((groups, n, rows, HD), BF16),
        pltpu.VMEM((groups, n - 1, rows, HD), BF16),
        pltpu.VMEM((groups, z * chunk, HD), BF16),
        pltpu.VMEM((groups, z - 1, chunk, HD), BF16),
        pltpu.VMEM((groups, chunk, HD), BF16),
        pltpu.VMEM((groups, z * chunk, HD), BF16),
        pltpu.SemaphoreType.DMA((5,)),
        pltpu.SemaphoreType.DMA((count,)),
        pltpu.SemaphoreType.DMA((count,)),
    ]
    return pl.pallas_call(
        functools.partial(kernel, sizes),
        out_shape=(
            jax.ShapeDtypeStruct(query_heads.shape, BF16),
            jax.ShapeDtypeStruct(key_heads.shape, BF16),
            jax.ShapeDtypeStruct(key_heads.shape, BF16),
            jax.ShapeDtypeStruct((1, rows, dt), BF16),
            jax.ShapeDtypeStruct((dn, cols), F32),
        ),
        in_specs=[smem, vmem, vmem, vmem] + [anywhere] * 5,
        out_specs=(vmem,) * 5,
        scratch_shapes=scratch,
        compiler_params=pltpu.CompilerParams(
            collective_id=0, has_side_effects=True, vmem_limit_bytes=56 * 1024 * 1024
        ),
    )(
        block_order, key_heads, value_heads, log_norm, hidden, query_heads, attention_out,
        output_grad, value_weight,
    )


def solution(mesh):
    placed = (
        P("dp", "ctx", None),
        P("dp", "ctx", "tp"),
        P("dp", "ctx", "tp"),
        P("dp", "ctx", "tp"),
        P("dp", "ctx", "tp"),
        P("dp", "ctx", "tp"),
        P("dp", "tp", "ctx"),
        P(),
        P(None, "tp"),
    )
    return jax.shard_map(
        shards,
        mesh=mesh,
        in_specs=placed,
        out_specs=(
            P("dp", "ctx", "tp"),
            P("dp", "ctx", "tp"),
            P("dp", "ctx", "tp"),
            P("dp", "ctx", "tp"),
            P("ctx", "tp"),
        ),
        check_vma=False,
    )
```

```python
import functools

import jax
import jax.numpy as jnp
from jax import lax
from jax.experimental import pallas as pl
from jax.experimental.pallas import tpu as pltpu
from jax.sharding import PartitionSpec as P

HD = 128
HQ = 32
KVH = 4
F32 = jnp.float32
BF16 = jnp.bfloat16
MESH = pl.DeviceIdType.MESH
VMEM_LIMIT = 60 * 1024 * 1024


def dot(a, b, ca, cb):
    return lax.dot_general(a, b, (((ca,), (cb,)), ((), ())), preferred_element_type=F32)


def kernel(
    sizes,
    order_ref, k_ref, v_ref, norm_ref, hid_ref, q_ref, ao_ref, og_ref, vw_ref,
    dq_ref, dk_ref, dv_ref, dh_ref, zall,
    qs, aos, ogs, kg, vg, hg, wg, ht, prob, acck, accv, bias,
    dvp, dvr, vown, vall, vtp, dkp, dkr, wp, zr, zown,
    local_sem, send, recv,
):
    n, t, z, rows, groups, members, dn, dt, chunk, keyc = sizes
    me, mt, mz = lax.axis_index("ctx"), lax.axis_index("tp"), lax.axis_index("dp")
    keys = n * rows
    blk = rows // 2
    scale = HD ** (-0.5)
    width = 2 * rows
    pairs = members // 2

    loads = [
        pltpu.make_async_copy(q_ref, qs, local_sem.at[0]),
        pltpu.make_async_copy(og_ref, ogs, local_sem.at[1]),
        pltpu.make_async_copy(ao_ref, aos, local_sem.at[2]),
        pltpu.make_async_copy(
            hid_ref.at[0, :, pl.ds(pl.multiple_of(me * dn, 128), dn)], hg.at[me], local_sem.at[3]
        ),
        pltpu.make_async_copy(
            vw_ref.at[pl.ds(pl.multiple_of(mt * dt, 128), dt)], wg.at[mt], local_sem.at[4]
        ),
    ]
    for load in loads:
        load.start()

    peers = {"ctx": (me, n), "tp": (mt, t), "dp": (mz, z)}

    def others(axis):
        mine, count = peers[axis]
        return [lax.rem(mine + o, count) for o in range(1, count)]

    barrier = pltpu.get_barrier_semaphore()
    for axis in peers:
        for peer in others(axis):
            pl.semaphore_signal(barrier, inc=1, device_id={axis: peer}, device_id_type=MESH)
    pl.semaphore_wait(barrier, n - 1 + t - 1 + z - 1)

    used = [0]

    def fan(axis, source, target):
        made = []
        for o, peer in enumerate(others(axis)):
            copy = pltpu.make_async_remote_copy(
                src_ref=source(peer),
                dst_ref=target(o),
                send_sem=send.at[used[0]],
                recv_sem=recv.at[used[0]],
                device_id={axis: peer},
                device_id_type=MESH,
            )
            used[0] += 1
            copy.start()
            made.append(copy)
        return made

    my_rows = pl.ds(pl.multiple_of(me * rows, rows), rows)
    k_copies = fan("ctx", lambda p: k_ref.at[0], lambda o: kg.at[my_rows])
    part = rows // t
    my_part = pl.ds(pl.multiple_of(mt * part, 16), part)
    h_copies = fan(
        "ctx",
        lambda p: hid_ref.at[0, my_part, pl.ds(pl.multiple_of(p * dn, 128), dn)],
        lambda o: hg.at[me, my_part],
    )
    half = dt // 2

    def weight_half(i):
        return fan(
            "tp",
            lambda p: vw_ref.at[pl.ds(pl.multiple_of(p * dt + i * half, 128), half)],
            lambda o: wg.at[mt, i * half : (i + 1) * half],
        )

    w_copies = weight_half(0)
    kg[my_rows] = k_ref[0]
    vg[my_rows] = v_ref[0]

    lane = lax.broadcasted_iota(jnp.int32, (blk, width), 1) % rows
    first = order_ref[2 * me] * blk
    second = order_ref[2 * me + 1] * blk
    query_pos = lane % blk + jnp.where(lane < blk, first, second)
    inside = lax.broadcasted_iota(jnp.int32, (blk, width), 0)
    for b in range(keys // blk):
        key_pos = inside + order_ref[b] * blk
        bias[b * blk : (b + 1) * blk] = jnp.where(key_pos <= query_pos, 0.0, -1e30).astype(F32)

    def two(ref, head):
        return jnp.concatenate(
            [ref[0, :, pl.ds(pl.multiple_of((head + j) * HD, HD), HD)] for j in range(2)], axis=0
        )

    def lanes(head):
        pieces = [norm_ref[0, pl.ds(head + j, 1), :] for j in range(2)]
        return jnp.concatenate(pieces, axis=1)

    loads[0].wait()
    loads[1].wait()
    for copy in k_copies:
        copy.wait_recv()

    def values(g):
        col = g * HD

        def pair(step, carry):
            head = g * members + step * 2
            q2, og2, norm = two(qs, head), two(ogs, head), lanes(head)

            def block(c, carry):
                at = pl.ds(pl.multiple_of(c * keyc, keyc), keyc)
                s = dot(kg[at, col : col + HD], q2, 1, 1) * scale
                p = jnp.exp(s + bias[at] - norm)
                prob[g * pairs + step, at] = p
                accv[g, at] += dot(p.astype(BF16), og2, 1, 0)
                return carry

            return lax.fori_loop(0, keys // keyc, block, carry)

        accv[g] = jnp.zeros((keys, HD), F32)
        lax.fori_loop(0, pairs, pair, 0)
        for s in range(n):
            dvp[g, s] = accv[g, s * rows : (s + 1) * rows].astype(BF16)
        return fan("ctx", lambda p: dvp.at[g, p], lambda o: dvr.at[g, o])

    def slopes(g):
        col = g * HD
        acck[g] = jnp.zeros((keys, HD), F32)

        def pair(step, carry):
            head = g * members + step * 2
            q2, og2 = two(qs, head), two(ogs, head)
            product = og2.astype(F32) * two(aos, head).astype(F32)
            delta = jnp.sum(product.T, axis=0, keepdims=True)

            def block(c, dq):
                at = pl.ds(pl.multiple_of(c * keyc, keyc), keyc)
                through = dot(vg[at, col : col + HD], og2, 1, 1)
                ds = (prob[g * pairs + step, at] * (through - delta)).astype(BF16)
                acck[g, at] += dot(ds, q2, 1, 0)
                return dq + dot(kg[at, col : col + HD].T, ds, 1, 0)

            dq = lax.fori_loop(0, keys // keyc, block, jnp.zeros((HD, width), F32))
            dq = (dq * scale).T.astype(BF16)
            for j in range(2):
                dq_ref[0, :, pl.ds(pl.multiple_of((head + j) * HD, HD), HD)] = dq[
                    j * rows : (j + 1) * rows
                ]
            return carry

        lax.fori_loop(0, pairs, pair, 0)
        for s in range(n):
            dkp[g, s] = acck[g, s * rows : (s + 1) * rows].astype(BF16)
        return fan("ctx", lambda p: dkp.at[g, p], lambda o: dkr.at[g, o])

    def reduced(copies, own, landed, g):
        for copy in copies:
            copy.wait_recv()
        total = own
        for o in range(n - 1):
            total = total + landed[g, o].astype(F32)
        return total

    def value_out(g, copies):
        col = g * HD
        total = reduced(copies, dvp[g, me].astype(F32), dvr, g).astype(BF16)
        dv_ref[0, :, col : col + HD] = total
        vown[g] = total
        made = fan("ctx", lambda p: vown.at[g], lambda o: vall.at[g, me])
        made_tp = fan("tp", lambda p: vown.at[g], lambda o: vtp.at[g, mt])
        vall[g, me] = total
        vtp[g, mt] = total
        return made, made_tp

    def weight_part(g, copies):
        for copy in copies:
            copy.wait_recv()
        size = min(dn, 256)

        def tile(i, carry):
            at = pl.ds(pl.multiple_of(i * size, size), size)
            rhs = vall[g].reshape(keys, HD)
            wp[g, at] = dot(ht[at], rhs, 1, 0).astype(BF16)
            return carry

        lax.fori_loop(0, dn // size, tile, 0)
        if z * chunk > dn:
            wp[g, dn:] = jnp.zeros((z * chunk - dn, HD), BF16)

        def piece(p):
            return wp.at[g, pl.ds(pl.multiple_of(p * chunk, 16), chunk)]

        return fan("dp", piece, lambda o: zr.at[g, o])

    def weight_sum(g, copies):
        for copy in copies:
            copy.wait_recv()
        mine = pl.ds(pl.multiple_of(mz * chunk, 16), chunk)
        total = wp[g, mine].astype(F32)
        for o in range(z - 1):
            total = total + zr[g, o].astype(F32)
        total = total.astype(BF16)
        zown[g] = total
        made = fan("dp", lambda p: zown.at[g], lambda o: zall.at[g, mine])
        zall[g, mine] = total
        return made

    dv_copies = [values(g) for g in range(groups)]
    v_copies = fan("ctx", lambda p: v_ref.at[0], lambda o: vg.at[my_rows])
    loads[3].wait()
    for copy in h_copies:
        copy.wait_recv()
    f_copies = []
    for source in others("ctx"):
        f_copies += fan(
            "tp",
            lambda p, source=source: hg.at[source, my_part],
            lambda o, source=source: hg.at[source, my_part],
        )
    w_copies += weight_half(1)
    gathers, shares, dk_copies, w_parts = [], [], [], []
    for g in range(groups):
        made, made_tp = value_out(g, dv_copies[g])
        gathers.append(made)
        shares.append(made_tp)
    loads[2].wait()
    for copy in v_copies:
        copy.wait_recv()
    dk_copies.append(slopes(0))
    for copy in f_copies:
        copy.wait_recv()
    for s in range(n):
        ht[:, s * rows : (s + 1) * rows] = hg[s].T
    for g in range(groups):
        w_parts.append(weight_part(g, gathers[g]))
    for g in range(1, groups):
        dk_copies.append(slopes(g))
    z_copies = [weight_sum(g, w_parts[g]) for g in range(groups)]

    loads[4].wait()
    for copy in w_copies:
        copy.wait_recv()
    for g in range(groups):
        for copy in shares[g]:
            copy.wait_recv()
    size = min(dt, 256)

    def out_tile(i, carry):
        at = pl.ds(pl.multiple_of(i * size, size), size)
        total = jnp.zeros((rows, size), F32)
        for p in range(t):
            lhs = jnp.concatenate([vtp[g, p] for g in range(groups)], axis=1)
            total = total + dot(lhs, wg[p, at], 1, 1)
        dh_ref[0, :, at] = total.astype(BF16)
        return carry

    lax.fori_loop(0, dt // size, out_tile, 0)

    for g in range(groups):
        col = g * HD
        total = reduced(dk_copies[g], dkp[g, me].astype(F32), dkr, g)
        dk_ref[0, :, col : col + HD] = (total * scale).astype(BF16)

    for g in range(groups):
        for copy in z_copies[g]:
            copy.wait_recv()

    everything = k_copies + v_copies + h_copies + w_copies + f_copies
    for group in dv_copies + gathers + shares + dk_copies + w_parts + z_copies:
        everything = everything + group
    for copy in everything:
        copy.wait_send()


def finish(norm, *refs):
    ins, outs, wide, sems = refs[:5], refs[5:10], refs[10], refs[11]
    copies = [pltpu.make_async_copy(ins[i], outs[i], sems.at[i]) for i in range(4)]
    for copy in copies:
        copy.start()
    total = ins[4]
    for g in range(total.shape[0]):
        wide[:, g * HD : (g + 1) * HD] = total[g, : wide.shape[0]].astype(F32) * norm
    copies.append(pltpu.make_async_copy(wide, outs[4], sems.at[4]))
    copies[4].start()
    for copy in copies:
        copy.wait()


def shards(
    hidden, query_heads, key_heads, value_heads, attention_out, output_grad,
    log_norm, block_order, value_weight,
):
    n, t, z = lax.axis_size("ctx"), lax.axis_size("tp"), lax.axis_size("dp")
    rows = query_heads.shape[1]
    depth = hidden.shape[2]
    cols = key_heads.shape[2]
    groups = cols // HD
    heads = query_heads.shape[2] // HD
    members = heads // groups
    dn, dt = depth // n, depth // t
    chunk = -(-dn // (16 * z)) * 16
    keys = n * rows
    keyc = min(keys, 512)
    sizes = (n, t, z, rows, groups, members, dn, dt, chunk, keyc)
    count = (n - 1) * (3 + 3 * groups + t - 1) + (t - 1) * (2 + groups) + (z - 1) * 2 * groups
    vmem, anywhere = pl.BlockSpec(memory_space=pltpu.VMEM), pl.BlockSpec(memory_space=pl.ANY)
    smem = pl.BlockSpec(memory_space=pltpu.SMEM)
    wide = (1, rows, heads * HD)
    scratch = [
        pltpu.VMEM(wide, BF16),
        pltpu.VMEM(wide, BF16),
        pltpu.VMEM(wide, BF16),
        pltpu.VMEM((keys, cols), BF16),
        pltpu.VMEM((keys, cols), BF16),
        pltpu.VMEM((n, rows, dn), BF16),
        pltpu.VMEM((t, dt, cols), BF16),
        pltpu.VMEM((dn, keys), BF16),
        pltpu.VMEM((heads // 2, keys, 2 * rows), F32),
        pltpu.VMEM((groups, keys, HD), F32),
        pltpu.VMEM((groups, keys, HD), F32),
        pltpu.VMEM((keys, 2 * rows), F32),
        pltpu.VMEM((groups, n, rows, HD), BF16),
        pltpu.VMEM((groups, n - 1, rows, HD), BF16),
        pltpu.VMEM((groups, rows, HD), BF16),
        pltpu.VMEM((groups, n, rows, HD), BF16),
        pltpu.VMEM((groups, t, rows, HD), BF16),
        pltpu.VMEM((groups, n, rows, HD), BF16),
        pltpu.VMEM((groups, n - 1, rows, HD), BF16),
        pltpu.VMEM((groups, z * chunk, HD), BF16),
        pltpu.VMEM((groups, z - 1, chunk, HD), BF16),
        pltpu.VMEM((groups, chunk, HD), BF16),
        pltpu.SemaphoreType.DMA((5,)),
        pltpu.SemaphoreType.DMA((count,)),
        pltpu.SemaphoreType.DMA((count,)),
    ]
    results = pl.pallas_call(
        functools.partial(kernel, sizes),
        out_shape=(
            pltpu.VMEM(query_heads.shape, BF16),
            pltpu.VMEM(key_heads.shape, BF16),
            pltpu.VMEM(key_heads.shape, BF16),
            pltpu.VMEM((1, rows, dt), BF16),
            pltpu.VMEM((groups, z * chunk, HD), BF16),
        ),
        in_specs=[smem, vmem, vmem, vmem] + [anywhere] * 5,
        out_specs=(vmem,) * 5,
        scratch_shapes=scratch,
        compiler_params=pltpu.CompilerParams(
            collective_id=0, has_side_effects=True, vmem_limit_bytes=VMEM_LIMIT
        ),
    )(
        block_order, key_heads, value_heads, log_norm, hidden, query_heads, attention_out,
        output_grad, value_weight,
    )
    return pl.pallas_call(
        functools.partial(finish, (z * n * rows) ** (-0.5)),
        out_shape=(
            jax.ShapeDtypeStruct(query_heads.shape, BF16),
            jax.ShapeDtypeStruct(key_heads.shape, BF16),
            jax.ShapeDtypeStruct(key_heads.shape, BF16),
            jax.ShapeDtypeStruct((1, rows, dt), BF16),
            jax.ShapeDtypeStruct((dn, cols), F32),
        ),
        in_specs=[vmem] * 5,
        out_specs=(anywhere,) * 5,
        scratch_shapes=[pltpu.VMEM((dn, cols), F32), pltpu.SemaphoreType.DMA((5,))],
    )(*results)


def solution(mesh):
    placed = (
        P("dp", "ctx", None),
        P("dp", "ctx", "tp"),
        P("dp", "ctx", "tp"),
        P("dp", "ctx", "tp"),
        P("dp", "ctx", "tp"),
        P("dp", "ctx", "tp"),
        P("dp", "tp", "ctx"),
        P(),
        P(None, "tp"),
    )
    return jax.shard_map(
        shards,
        mesh=mesh,
        in_specs=placed,
        out_specs=(
            P("dp", "ctx", "tp"),
            P("dp", "ctx", "tp"),
            P("dp", "ctx", "tp"),
            P("dp", "ctx", "tp"),
            P("ctx", "tp"),
        ),
        check_vma=False,
    )
```

```python
import functools

import jax
import jax.numpy as jnp
from jax import lax
from jax.experimental import pallas as pl
from jax.experimental.pallas import tpu as pltpu
from jax.sharding import PartitionSpec as P

HD = 128
HQ = 32
KVH = 4
F32 = jnp.float32
BF16 = jnp.bfloat16
MESH = pl.DeviceIdType.MESH
VMEM_LIMIT = 60 * 1024 * 1024


def dot(a, b, ca, cb):
    return lax.dot_general(a, b, (((ca,), (cb,)), ((), ())), preferred_element_type=F32)


def kernel(
    sizes,
    order_ref, k_ref, v_ref, norm_ref, hid_ref, q_ref, ao_ref, og_ref, vw_ref,
    dq_ref, dk_ref, dv_ref, dh_ref, zall,
    qs, aos, ogs, kg, vg, hg, wg, ht, prob, acck, accv, bias,
    dvp, dvr, vown, vall, vtp, dkp, dkr, wp, zr, zs, zacc,
    local_sem, send, recv, zsend, zrecv,
):
    n, t, z, rows, groups, members, dn, dt, chunk, keyc = sizes
    me, mt, mz = lax.axis_index("ctx"), lax.axis_index("tp"), lax.axis_index("dp")
    keys = n * rows
    blk = rows // 2
    scale = HD ** (-0.5)
    width = 2 * rows
    pairs = members // 2

    loads = [
        pltpu.make_async_copy(q_ref, qs, local_sem.at[0]),
        pltpu.make_async_copy(og_ref, ogs, local_sem.at[1]),
        pltpu.make_async_copy(ao_ref, aos, local_sem.at[2]),
        pltpu.make_async_copy(
            hid_ref.at[0, :, pl.ds(pl.multiple_of(me * dn, 128), dn)], hg.at[me], local_sem.at[3]
        ),
        pltpu.make_async_copy(
            vw_ref.at[pl.ds(pl.multiple_of(mt * dt, 128), dt)], wg.at[mt], local_sem.at[4]
        ),
    ]
    for load in loads:
        load.start()

    peers = {"ctx": (me, n), "tp": (mt, t), "dp": (mz, z)}

    def others(axis):
        mine, count = peers[axis]
        return [lax.rem(mine + o, count) for o in range(1, count)]

    barrier = pltpu.get_barrier_semaphore()
    for axis in peers:
        for peer in others(axis):
            pl.semaphore_signal(barrier, inc=1, device_id={axis: peer}, device_id_type=MESH)
    pl.semaphore_wait(barrier, n - 1 + t - 1 + z - 1)

    used = [0]

    def fan(axis, source, target):
        made = []
        for o, peer in enumerate(others(axis)):
            copy = pltpu.make_async_remote_copy(
                src_ref=source(peer),
                dst_ref=target(o),
                send_sem=send.at[used[0]],
                recv_sem=recv.at[used[0]],
                device_id={axis: peer},
                device_id_type=MESH,
            )
            used[0] += 1
            copy.start()
            made.append(copy)
        return made

    my_rows = pl.ds(pl.multiple_of(me * rows, rows), rows)
    k_copies = fan("ctx", lambda p: k_ref.at[0], lambda o: kg.at[my_rows])
    part = rows // t
    my_part = pl.ds(pl.multiple_of(mt * part, 16), part)
    half = dt // 2
    parity = me % 2
    hops = n // 2
    near = me + 1 - 2 * parity
    fars = [(k, c) for k in range(1, hops) for c in range(2)]

    def far(k, c):
        return lax.rem(me // 2 + k + hops, hops) * 2 + lax.rem(parity + c + 2, 2)

    def one(axis, peer, source, target):
        copy = pltpu.make_async_remote_copy(
            src_ref=source,
            dst_ref=target,
            send_sem=send.at[used[0]],
            recv_sem=recv.at[used[0]],
            device_id={axis: peer},
            device_id_type=MESH,
        )
        used[0] += 1
        copy.start()
        return copy

    def columns(p):
        return pl.ds(pl.multiple_of(p * dn, 128), dn)

    h_copies = [
        one("ctx", far(k, c), hid_ref.at[0, my_part, columns(far(k, c))], hg.at[me, my_part])
        for k, c in fars
    ]
    near_copy = one("ctx", near, hid_ref.at[0, :, columns(near)], hg.at[me])
    kg[my_rows] = k_ref[0]
    vg[my_rows] = v_ref[0]

    lane = lax.broadcasted_iota(jnp.int32, (blk, width), 1) % rows
    first = order_ref[2 * me] * blk
    second = order_ref[2 * me + 1] * blk
    query_pos = lane % blk + jnp.where(lane < blk, first, second)
    inside = lax.broadcasted_iota(jnp.int32, (blk, width), 0)
    for b in range(keys // blk):
        key_pos = inside + order_ref[b] * blk
        bias[b * blk : (b + 1) * blk] = jnp.where(key_pos <= query_pos, 0.0, -1e30).astype(F32)

    def two(ref, head):
        return jnp.concatenate(
            [ref[0, :, pl.ds(pl.multiple_of((head + j) * HD, HD), HD)] for j in range(2)], axis=0
        )

    def lanes(head):
        pieces = [norm_ref[0, pl.ds(head + j, 1), :] for j in range(2)]
        return jnp.concatenate(pieces, axis=1)

    loads[0].wait()
    loads[1].wait()
    for copy in k_copies:
        copy.wait_recv()

    def values(g):
        col = g * HD

        def pair(step, carry):
            head = g * members + step * 2
            q2, og2, norm = two(qs, head), two(ogs, head), lanes(head)

            def block(c, carry):
                at = pl.ds(pl.multiple_of(c * keyc, keyc), keyc)
                s = dot(kg[at, col : col + HD], q2, 1, 1) * scale
                p = jnp.exp(s + bias[at] - norm)
                prob[g * pairs + step, at] = p
                accv[g, at] += dot(p.astype(BF16), og2, 1, 0)
                return carry

            return lax.fori_loop(0, keys // keyc, block, carry)

        accv[g] = jnp.zeros((keys, HD), F32)
        lax.fori_loop(0, pairs, pair, 0)
        for s in range(n):
            dvp[g, s] = accv[g, s * rows : (s + 1) * rows].astype(BF16)
        return fan("ctx", lambda p: dvp.at[g, p], lambda o: dvr.at[g, o])

    def slopes(g):
        col = g * HD
        acck[g] = jnp.zeros((keys, HD), F32)

        def pair(step, carry):
            head = g * members + step * 2
            q2, og2 = two(qs, head), two(ogs, head)
            product = og2.astype(F32) * two(aos, head).astype(F32)
            delta = jnp.sum(product.T, axis=0, keepdims=True)

            def block(c, dq):
                at = pl.ds(pl.multiple_of(c * keyc, keyc), keyc)
                through = dot(vg[at, col : col + HD], og2, 1, 1)
                ds = (prob[g * pairs + step, at] * (through - delta)).astype(BF16)
                acck[g, at] += dot(ds, q2, 1, 0)
                return dq + dot(kg[at, col : col + HD].T, ds, 1, 0)

            dq = lax.fori_loop(0, keys // keyc, block, jnp.zeros((HD, width), F32))
            dq = (dq * scale).T.astype(BF16)
            for j in range(2):
                dq_ref[0, :, pl.ds(pl.multiple_of((head + j) * HD, HD), HD)] = dq[
                    j * rows : (j + 1) * rows
                ]
            return carry

        lax.fori_loop(0, pairs, pair, 0)
        for s in range(n):
            dkp[g, s] = acck[g, s * rows : (s + 1) * rows].astype(BF16)
        return fan("ctx", lambda p: dkp.at[g, p], lambda o: dkr.at[g, o])

    def reduced(copies, own, landed, g):
        for copy in copies:
            copy.wait_recv()
        total = own
        for o in range(n - 1):
            total = total + landed[g, o].astype(F32)
        return total

    def value_out(g, copies):
        col = g * HD
        total = reduced(copies, dvp[g, me].astype(F32), dvr, g).astype(BF16)
        dv_ref[0, :, col : col + HD] = total
        vown[g] = total
        made = fan("ctx", lambda p: vown.at[g], lambda o: vall.at[g, me])
        made_tp = fan("tp", lambda p: vown.at[g], lambda o: vtp.at[g, mt])
        vall[g, me] = total
        vtp[g, mt] = total
        return made, made_tp

    def weight_part(g, copies):
        for copy in copies:
            copy.wait_recv()
        size = min(dn, 256)

        def tile(i, carry):
            at = pl.ds(pl.multiple_of(i * size, size), size)
            rhs = vall[g].reshape(keys, HD)
            wp[g, at] = dot(ht[at], rhs, 1, 0).astype(BF16)
            return carry

        lax.fori_loop(0, dn // size, tile, 0)
        if z * chunk > dn:
            wp[g, dn:] = jnp.zeros((z * chunk - dn, HD), BF16)

    def hop(source, target, phase, flow, g, index):
        to = lax.rem(mz + 1, z) if flow == 0 else lax.rem(mz + z - 1, z)
        return pltpu.make_async_remote_copy(
            src_ref=source,
            dst_ref=target,
            send_sem=zsend.at[phase, flow, g, index],
            recv_sem=zrecv.at[phase, flow, g, index],
            device_id={"dp": to},
            device_id_type=MESH,
        )

    def sender(flow, owner):
        return mz < owner if flow == 0 else mz > owner

    def inner(flow):
        return mz > 0 if flow == 0 else mz < z - 1

    def outer(flow):
        return mz < z - 1 if flow == 0 else mz > 0

    def sum_hop(flow, g, owner):
        return hop(zs.at[flow, g, owner], zr.at[flow, g, owner], 0, flow, g, owner)

    def line_step(flow, g, owner):
        mine = slice(owner * chunk, (owner + 1) * chunk)

        @pl.when(sender(flow, owner))
        def _():
            zs[flow, g, owner] = wp[g, mine]

            @pl.when(inner(flow))
            def _():
                sum_hop(flow, g, owner).wait_recv()
                total = wp[g, mine].astype(F32) + zr[flow, g, owner].astype(F32)
                zs[flow, g, owner] = total.astype(BF16)

            sum_hop(flow, g, owner).start()

    def block_of(index):
        return pl.ds(pl.multiple_of(index * chunk, 16), chunk)

    def spread_hop(flow, g, index):
        at = block_of(index)
        return hop(zall.at[g, at], zall.at[g, at], 1, flow, g, index)

    def line_own(g):
        zacc[...] = wp[g, block_of(mz)].astype(F32)
        for flow in range(2):

            @pl.when(inner(flow))
            def _():
                sum_hop(flow, g, mz).wait_recv()
                zacc[...] += zr[flow, g, mz].astype(F32)

        zall[g, block_of(mz)] = zacc[...].astype(BF16)
        for flow in range(2):

            @pl.when(outer(flow))
            def _():
                spread_hop(flow, g, mz).start()

    def line_pass(flow, g, d):
        there = mz >= d if flow == 0 else mz + d < z

        @pl.when(there)
        def _():
            index = mz - d if flow == 0 else mz + d
            spread_hop(flow, g, index).wait_recv()

            @pl.when(outer(flow))
            def _():
                spread_hop(flow, g, index).start()

    def line_drain():
        for flow in range(2):
            for g in range(groups):
                for owner in range(z):

                    @pl.when(sender(flow, owner))
                    def _():
                        sum_hop(flow, g, owner).wait_send()

                    passed = mz >= owner if flow == 0 else mz <= owner

                    @pl.when(jnp.logical_and(passed, outer(flow)))
                    def _():
                        spread_hop(flow, g, owner).wait_send()

    dv_copies = [values(g) for g in range(groups)]
    f_copies = []
    for (k, c), copy in zip(fars, h_copies):
        copy.wait_recv()
        source = far(-k, -c)
        f_copies += fan(
            "tp",
            lambda p: hg.at[source, my_part],
            lambda o: hg.at[source, my_part],
        )
    my_half = pl.ds(pl.multiple_of(parity * half, 16), half)
    w_copies = fan(
        "tp",
        lambda p: vw_ref.at[pl.ds(pl.multiple_of(p * dt + parity * half, 16), half)],
        lambda o: wg.at[mt, my_half],
    )
    gathers, shares = [], []
    for g in range(groups):
        made, made_tp = value_out(g, dv_copies[g])
        gathers.append(made)
        shares.append(made_tp)
    v_copies = fan("ctx", lambda p: v_ref.at[0], lambda o: vg.at[my_rows])
    loads[3].wait()
    near_copy.wait_recv()
    for copy in f_copies:
        copy.wait_recv()
    for s in range(n):
        ht[:, s * rows : (s + 1) * rows] = hg[s].T
    for g in range(groups):
        weight_part(g, gathers[g])

    def line_round(j):
        for g in range(groups):
            line_step(0, g, z - 1 - j)
            line_step(1, g, j)

    loads[2].wait()
    for copy in v_copies:
        copy.wait_recv()
    line_round(0)
    dk_copies = [slopes(0)]
    for j in range(1, z - 1):
        line_round(j)
    for g in range(1, groups):
        dk_copies.append(slopes(g))
    for g in range(groups):
        line_own(g)
    for copy in w_copies:
        copy.wait_recv()
    relays = []
    for o in range(1, t):
        source = lax.rem(mt + t - o, t)
        relays.append(one("ctx", near, wg.at[source, my_half], wg.at[source, my_half]))
    for d in range(1, z):
        for g in range(groups):
            for flow in range(2):
                line_pass(flow, g, d)

    loads[4].wait()
    for copy in relays:
        copy.wait_recv()
    for g in range(groups):
        for copy in shares[g]:
            copy.wait_recv()
    size = min(dt, 256)

    def out_tile(i, carry):
        at = pl.ds(pl.multiple_of(i * size, size), size)
        total = jnp.zeros((rows, size), F32)
        for p in range(t):
            lhs = jnp.concatenate([vtp[g, p] for g in range(groups)], axis=1)
            total = total + dot(lhs, wg[p, at], 1, 1)
        dh_ref[0, :, at] = total.astype(BF16)
        return carry

    lax.fori_loop(0, dt // size, out_tile, 0)

    for g in range(groups):
        col = g * HD
        total = reduced(dk_copies[g], dkp[g, me].astype(F32), dkr, g)
        dk_ref[0, :, col : col + HD] = (total * scale).astype(BF16)

    line_drain()
    everything = k_copies + v_copies + h_copies + w_copies + f_copies + relays + [near_copy]
    for group in dv_copies + gathers + shares + dk_copies:
        everything = everything + group
    for copy in everything:
        copy.wait_send()


def finish(norm, *refs):
    ins, outs, wide, sems = refs[:5], refs[5:10], refs[10], refs[11]
    copies = [pltpu.make_async_copy(ins[i], outs[i], sems.at[i]) for i in range(4)]
    for copy in copies:
        copy.start()
    total = ins[4]
    for g in range(total.shape[0]):
        wide[:, g * HD : (g + 1) * HD] = total[g, : wide.shape[0]].astype(F32) * norm
    copies.append(pltpu.make_async_copy(wide, outs[4], sems.at[4]))
    copies[4].start()
    for copy in copies:
        copy.wait()


def shards(
    hidden, query_heads, key_heads, value_heads, attention_out, output_grad,
    log_norm, block_order, value_weight,
):
    n, t, z = lax.axis_size("ctx"), lax.axis_size("tp"), lax.axis_size("dp")
    rows = query_heads.shape[1]
    depth = hidden.shape[2]
    cols = key_heads.shape[2]
    groups = cols // HD
    heads = query_heads.shape[2] // HD
    members = heads // groups
    dn, dt = depth // n, depth // t
    chunk = -(-dn // (16 * z)) * 16
    keys = n * rows
    keyc = min(keys, 512)
    sizes = (n, t, z, rows, groups, members, dn, dt, chunk, keyc)
    count = (n - 1) * (3 + 3 * groups + t - 1) + (t - 1) * (2 + groups)
    vmem, anywhere = pl.BlockSpec(memory_space=pltpu.VMEM), pl.BlockSpec(memory_space=pltpu.HBM)
    smem = pl.BlockSpec(memory_space=pltpu.SMEM)
    wide = (1, rows, heads * HD)
    scratch = [
        pltpu.VMEM(wide, BF16),
        pltpu.VMEM(wide, BF16),
        pltpu.VMEM(wide, BF16),
        pltpu.VMEM((keys, cols), BF16),
        pltpu.VMEM((keys, cols), BF16),
        pltpu.VMEM((n, rows, dn), BF16),
        pltpu.VMEM((t, dt, cols), BF16),
        pltpu.VMEM((dn, keys), BF16),
        pltpu.VMEM((heads // 2, keys, 2 * rows), F32),
        pltpu.VMEM((groups, keys, HD), F32),
        pltpu.VMEM((groups, keys, HD), F32),
        pltpu.VMEM((keys, 2 * rows), F32),
        pltpu.VMEM((groups, n, rows, HD), BF16),
        pltpu.VMEM((groups, n - 1, rows, HD), BF16),
        pltpu.VMEM((groups, rows, HD), BF16),
        pltpu.VMEM((groups, n, rows, HD), BF16),
        pltpu.VMEM((groups, t, rows, HD), BF16),
        pltpu.VMEM((groups, n, rows, HD), BF16),
        pltpu.VMEM((groups, n - 1, rows, HD), BF16),
        pltpu.VMEM((groups, z * chunk, HD), BF16),
        pltpu.VMEM((2, groups, z, chunk, HD), BF16),
        pltpu.VMEM((2, groups, z, chunk, HD), BF16),
        pltpu.VMEM((chunk, HD), F32),
        pltpu.SemaphoreType.DMA((5,)),
        pltpu.SemaphoreType.DMA((count,)),
        pltpu.SemaphoreType.DMA((count,)),
        pltpu.SemaphoreType.DMA((2, 2, groups, z)),
        pltpu.SemaphoreType.DMA((2, 2, groups, z)),
    ]
    results = pl.pallas_call(
        functools.partial(kernel, sizes),
        out_shape=(
            pltpu.VMEM(query_heads.shape, BF16),
            pltpu.VMEM(key_heads.shape, BF16),
            pltpu.VMEM(key_heads.shape, BF16),
            pltpu.VMEM((1, rows, dt), BF16),
            pltpu.VMEM((groups, z * chunk, HD), BF16),
        ),
        in_specs=[smem, vmem, vmem, vmem] + [anywhere] * 5,
        out_specs=(vmem,) * 5,
        scratch_shapes=scratch,
        compiler_params=pltpu.CompilerParams(
            collective_id=0, has_side_effects=True, vmem_limit_bytes=VMEM_LIMIT
        ),
    )(
        block_order, key_heads, value_heads, log_norm, hidden, query_heads, attention_out,
        output_grad, value_weight,
    )
    return pl.pallas_call(
        functools.partial(finish, (z * n * rows) ** (-0.5)),
        out_shape=(
            jax.ShapeDtypeStruct(query_heads.shape, BF16),
            jax.ShapeDtypeStruct(key_heads.shape, BF16),
            jax.ShapeDtypeStruct(key_heads.shape, BF16),
            jax.ShapeDtypeStruct((1, rows, dt), BF16),
            jax.ShapeDtypeStruct((dn, cols), F32),
        ),
        in_specs=[vmem] * 5,
        out_specs=(anywhere,) * 5,
        scratch_shapes=[pltpu.VMEM((dn, cols), F32), pltpu.SemaphoreType.DMA((5,))],
        compiler_params=pltpu.CompilerParams(vmem_limit_bytes=16 * 1024 * 1024),
    )(*results)


def solution(mesh):
    placed = (
        P("dp", "ctx", None),
        P("dp", "ctx", "tp"),
        P("dp", "ctx", "tp"),
        P("dp", "ctx", "tp"),
        P("dp", "ctx", "tp"),
        P("dp", "ctx", "tp"),
        P("dp", "tp", "ctx"),
        P(),
        P(None, "tp"),
    )
    return jax.shard_map(
        shards,
        mesh=mesh,
        in_specs=placed,
        out_specs=(
            P("dp", "ctx", "tp"),
            P("dp", "ctx", "tp"),
            P("dp", "ctx", "tp"),
            P("dp", "ctx", "tp"),
            P("ctx", "tp"),
        ),
        check_vma=False,
    )
```
